32 devices in a mesh: sec: 2 (over y), ty: 16 (over z, x, core).
Axes of the slice: x: 2, y: 2, z: 4, core: 2. Of those that a mesh axis runs over, the one named last changes fastest.
Arguments:
- points: float32 [4, 32768], P(None, ('sec', 'ty')), parts along dimension 1, may hold values from -88 to 2136, as said below
- source: bfloat16 [1024, 2048], P(('sec', 'ty')), parts along dimension 0, may hold values from -4 to 4
- slab_first: int32 [32], P(('sec', 'ty')), parts along dimension 0, may hold values from 0 to 29, as said below
- slab_count: int32 [32], P(('sec', 'ty')), parts along dimension 0, may hold values from 3 to 6, as said below
Outputs:
- rendered: bfloat16 [1024, 2048], P(('sec', 'ty')), parts along dimension 0
- vertex_affines: float32 [6, 128, 256], P(None, ('sec', 'ty')), parts along dimension 1
The draws below stay inside these ranges and needn't reach their ends.
There are 2 independent parts, one for each index of `sec`. The reference program is written for one: setup_inputs(seed, part) draws one part's arguments, and reference() takes and returns one part's arrays. A program takes and returns all parts, laid end to end along the dimension named above; each array names one. Nothing has to cross between parts.
Inputs may be any that keep to these rules, and one draw needn't show every extreme that they name: `points`: for tile t, rows 0 and 1 are fixed positions: each 16 x 16 pixel cell of rows t*32 to (t+1)*32 and columns 0 to 2048 holds 4 of them, listed cell by cell, cells in row-major order; rows 2 and 3 are the matching moving positions. Source block j is rows j*16 to (j+1)*16 - 1. Tile t samples blocks slab_first[t] to slab_first[t] + slab_count[t] - 1, all within rows (t-1)*32 to (t+2)*32 - 1. slab_count reaches 6 on some tile in every draw.
All inputs are finite; a program needn't handle non-finite values.
Results may differ from the reference program's by a relative error of at most 0.008.
Values may be sent and summed in bfloat16 or wider, within the bound.
A program may use at most 64 MiB of HBM per device.

```python
import jax
import jax.numpy as jnp
from jax import lax

W = 2048
BH = 16
NB = 2
PC = 4
SP = 8
H = 32
K = 6
P_SIZE = 1024
VR = 4
VC = 256
ROWS = 512
N_TY = 16


def strip_shifts(key):
    first_key, second_key = jax.random.split(jax.random.fold_in(key, 31))
    strip_ids = jnp.arange(N_TY, dtype=jnp.int32)
    shifts = jax.random.randint(first_key, (N_TY,), -1, 2, dtype=jnp.int32)
    chosen = jax.random.randint(second_key, (), 1, N_TY - 2, dtype=jnp.int32)
    shifts = jnp.where(strip_ids == chosen, -1, jnp.where(strip_ids == chosen + 1, 1, shifts))
    shifts = jnp.where(strip_ids == 0, jnp.maximum(shifts, 0), shifts)
    shifts = jnp.where(strip_ids == N_TY - 1, jnp.minimum(shifts, 0), shifts)
    return shifts


def slab_bounds(key):
    shifts = strip_shifts(key)
    strip_ids = jnp.arange(N_TY, dtype=jnp.int32)
    from_above = jnp.concatenate([shifts[:1], shifts[:-1]])
    from_below = jnp.concatenate([shifts[1:], shifts[-1:]])
    lowest = jnp.minimum(jnp.minimum(from_above, shifts), from_below)
    highest = jnp.maximum(jnp.maximum(from_above, shifts), from_below)
    first_slab = jnp.maximum(0, jnp.maximum((strip_ids - 1) * NB, (strip_ids + lowest) * NB - 1))
    end_slab = jnp.minimum(N_TY * NB, jnp.minimum((strip_ids + 2) * NB, (strip_ids + 1 + highest) * NB + 1))
    return (first_slab, end_slab - first_slab)


def draw_slab_first(key, part):
    return slab_bounds(key)[0]


def draw_slab_count(key, part):
    return slab_bounds(key)[1]


def draw_points(key, part):
    shifts = strip_shifts(key).astype(jnp.float32)
    subkeys = jax.random.split(jax.random.fold_in(key, 57), 5)
    cell_cols = W // 16
    point_id = jnp.arange(N_TY * P_SIZE, dtype=jnp.int32)
    strip_id = point_id // P_SIZE
    cell_id = point_id % P_SIZE // PC
    base_x = (cell_id % cell_cols * 16).astype(jnp.float32)
    base_y = (strip_id * H + cell_id // cell_cols * 16).astype(jnp.float32)
    jitter = jax.random.uniform(subkeys[0], (2, N_TY * P_SIZE), minval=0.0, maxval=16.0)
    fixed_x = base_x + jitter[0]
    fixed_y = base_y + jitter[1]
    stretch = jax.random.uniform(subkeys[1], (N_TY,), minval=-0.03, maxval=0.03)
    sideways = jax.random.uniform(subkeys[2], (N_TY,), minval=-16.0, maxval=16.0)
    shear_y = jax.random.uniform(subkeys[3], (N_TY,), minval=-0.004, maxval=0.004)
    wobble = jnp.clip(jax.random.normal(subkeys[4], (2, N_TY * P_SIZE)), -3.0, 3.0)
    centre = W / 2.0
    moved_x = centre + (1.0 + stretch[strip_id]) * (fixed_x - centre) + sideways[strip_id] + wobble[0]
    moved_y = fixed_y + shifts[strip_id] * H + shear_y[strip_id] * (fixed_x - centre) + wobble[1]
    return jnp.stack([fixed_x, fixed_y, moved_x, moved_y]).astype(jnp.float32)


def block_scale(own_key, shape, cuts, low, high):
    gain = 1.0
    for dim, blocks in cuts:
        draws = jax.random.uniform(jax.random.fold_in(jax.random.fold_in(own_key, 6), dim), (blocks,), jnp.float32, low / len(cuts), high / len(cuts))
        gain = gain * jnp.repeat(jnp.exp(draws), shape[dim] // blocks).reshape((-1,) + (1,) * (len(shape) - 1 - dim))
    return gain


def bell_draw(own_key, extent, deviation, most, cuts=(), kind=jnp.bfloat16):
    drawn = deviation * jax.random.normal(own_key, extent, jnp.float32)
    if cuts:
        drawn = drawn * block_scale(own_key, extent, cuts, -0.22, 0.18)
    return jnp.clip(drawn, -most, most).astype(kind)


def setup_inputs(seed: int = 0, part: int = 0) -> dict:
    splits = jax.random.split(jax.random.key(seed), 5)
    part_splits = jax.random.split(jax.random.fold_in(splits[4], part), 5)
    points = draw_points(jax.random.fold_in(jax.random.fold_in(splits[4], part), 71), part)
    source = bell_draw(part_splits[1], (ROWS, W), 1.0, 4.0, ((0, 16),))
    slab_first = draw_slab_first(jax.random.fold_in(jax.random.fold_in(splits[4], part), 71), part)
    slab_count = draw_slab_count(jax.random.fold_in(jax.random.fold_in(splits[4], part), 71), part)
    return {"points": points, "source": source, "slab_first": slab_first, "slab_count": slab_count}


PRECISE = lax.Precision.HIGHEST
RIDGE_TERM = 0.01


def solve_affine(moments, vertex_x, vertex_y):
    mass = moments[0]
    mean_px = moments[1] / mass
    mean_py = moments[2] / mass
    mean_qx = moments[3] / mass
    mean_qy = moments[4] / mass
    cov_xx = moments[5] / mass - mean_px * mean_px + RIDGE_TERM
    cov_xy = moments[6] / mass - mean_px * mean_py
    cov_yy = moments[7] / mass - mean_py * mean_py + RIDGE_TERM
    cross_xx = moments[8] / mass - mean_qx * mean_px
    cross_xy = moments[9] / mass - mean_qx * mean_py
    cross_yx = moments[10] / mass - mean_qy * mean_px
    cross_yy = moments[11] / mass - mean_qy * mean_py
    determ = cov_xx * cov_yy - cov_xy * cov_xy
    lin_xx = (cross_xx * cov_yy - cross_xy * cov_xy) / determ
    lin_xy = (cross_xy * cov_xx - cross_xx * cov_xy) / determ
    lin_yx = (cross_yx * cov_yy - cross_yy * cov_xy) / determ
    lin_yy = (cross_yy * cov_xx - cross_yx * cov_xy) / determ
    delta_x = vertex_x - mean_px
    delta_y = vertex_y - mean_py
    shift_x = mean_qx + lin_xx * delta_x + lin_xy * delta_y - vertex_x
    shift_y = mean_qy + lin_yx * delta_x + lin_yy * delta_y - vertex_y
    return jnp.stack([lin_xx, lin_xy, lin_yx, lin_yy, shift_x, shift_y])


def block_moments(pts, usable, strip_id):
    block_count = W // 128
    per_block = VC // block_count
    cell_rows = pts.shape[1] // (block_count * 8 * PC)
    grid = pts.reshape(4, cell_rows, block_count, 8 * PC)
    live = usable.reshape(cell_rows, block_count, 8 * PC)
    grid = jnp.pad(grid, ((0, 0), (0, 0), (1, 1), (0, 0)))
    live = jnp.pad(live, ((0, 0), (1, 1), (0, 0)))
    near = jnp.concatenate([grid[:, :, 0:block_count], grid[:, :, 1:block_count + 1],
                            grid[:, :, 2:block_count + 2]], axis=3)
    near_live = jnp.concatenate([live[:, 0:block_count], live[:, 1:block_count + 1],
                                 live[:, 2:block_count + 2]], axis=2)
    near = jnp.transpose(near, (0, 2, 1, 3)).reshape(4, block_count, cell_rows * 24 * PC)
    near_live = jnp.transpose(near_live, (1, 0, 2)).reshape(block_count, cell_rows * 24 * PC)
    centre_y = strip_id.astype(jnp.float32) * H + H / 2.0
    anchor = jnp.arange(block_count, dtype=jnp.float32) * 128.0 + 64.0
    fixed_x = (near[0] - anchor[:, None]) / H
    fixed_y = (near[1] - centre_y) / H
    moved_x = (near[2] - anchor[:, None]) / H
    moved_y = (near[3] - centre_y) / H
    unit_row = jnp.ones_like(fixed_x)
    features = jnp.stack([unit_row, fixed_x, fixed_y, moved_x, moved_y, fixed_x * fixed_x, fixed_x * fixed_y,
                          fixed_y * fixed_y, moved_x * fixed_x, moved_x * fixed_y, moved_y * fixed_x,
                          moved_y * fixed_y], axis=1) * near_live[:, None, :]
    vertex_col = jnp.arange(VC, dtype=jnp.float32).reshape(block_count, per_block) * SP + SP / 2.0
    vertex_row = jnp.arange(VR, dtype=jnp.float32) * SP + SP / 2.0 - H / 2.0
    gap_x = (near[0][:, :, None] - vertex_col[:, None, :]) / H
    gap_y = fixed_y[:, :, None] - (vertex_row / H)[None, None, :]
    weight_x = jnp.exp(-2.0 * gap_x * gap_x)
    weight_y = jnp.exp(-2.0 * gap_y * gap_y)
    weighted = features[:, :, None, :] * jnp.transpose(weight_y, (0, 2, 1))[:, None, :, :]
    moments = jnp.einsum("bkrm,bmc->bkrc", weighted, weight_x, precision=PRECISE)
    return jnp.transpose(moments, (1, 2, 0, 3)).reshape(12, VR, VC)


def vertex_frame():
    block_count = W // 128
    per_block = VC // block_count
    anchor = jnp.arange(block_count, dtype=jnp.float32) * 128.0 + 64.0
    vertex_col = jnp.arange(VC, dtype=jnp.float32) * SP + SP / 2.0
    vertex_row = jnp.arange(VR, dtype=jnp.float32) * SP + SP / 2.0 - H / 2.0
    column_anchor = jnp.repeat(anchor, per_block)
    vertex_x = jnp.broadcast_to(((vertex_col - column_anchor) / H)[None, :], (VR, VC))
    vertex_y = jnp.broadcast_to((vertex_row / H)[:, None], (VR, VC))
    return vertex_x, vertex_y


def tent_tables():
    row_local = jnp.arange(H, dtype=jnp.float32)
    ext_row = (jnp.arange(VR + 2, dtype=jnp.float32) - 1.0) * SP + SP / 2.0
    tent_rows = jnp.maximum(0.0, 1.0 - jnp.abs(row_local[:, None] - ext_row[None, :]) / SP)
    column = jnp.clip(jnp.arange(W, dtype=jnp.float32), SP / 2.0, W - SP / 2.0)
    vertex_col = jnp.arange(VC, dtype=jnp.float32) * SP + SP / 2.0
    tent_cols = jnp.maximum(0.0, 1.0 - jnp.abs(column[None, :] - vertex_col[:, None]) / SP)
    return tent_rows, tent_cols


def displace(near_shift, tent_rows, tent_cols):
    first_part = jnp.dot(jnp.dot(tent_rows, near_shift[0], precision=PRECISE), tent_cols, precision=PRECISE)
    second_part = jnp.dot(jnp.dot(tent_rows, near_shift[1], precision=PRECISE), tent_cols, precision=PRECISE)
    return jnp.stack([first_part, second_part])


def render_strip(slab_rows, first_slab, slab_total, disp, strip_id):
    block_count = W // 128
    samp_y = jnp.arange(H, dtype=jnp.float32)[:, None] + H * disp[1]
    samp_x = jnp.arange(W, dtype=jnp.float32)[None, :] + H * disp[0]
    slot_ids = jnp.arange(K, dtype=jnp.int32)
    slot_row = (first_slab + slot_ids) * BH - strip_id * H
    row_pos = (slot_row[:, None] + jnp.arange(BH, dtype=jnp.int32)[None, :]).reshape(K * BH).astype(jnp.float32)
    slot_live = jnp.repeat((slot_ids < slab_total).astype(jnp.float32), BH)
    padded = jnp.pad(slab_rows, ((0, 0), (64, 192)))
    blocks = padded.reshape(K * BH, block_count + 2, 128)
    windows = jnp.concatenate([blocks[:, :block_count], blocks[:, 1:block_count + 1]], axis=2)
    windows = jnp.transpose(windows, (1, 0, 2))
    block_y = samp_y.reshape(H, block_count, 128).transpose(1, 0, 2).reshape(block_count, H * 128)
    block_x = samp_x.reshape(H, block_count, 128).transpose(1, 0, 2).reshape(block_count, H * 128)
    block_ids = jnp.arange(block_count, dtype=jnp.int32)

    def one_block(packed):
        along_y, along_x, window, block_id = packed
        col_pos = block_id.astype(jnp.float32) * 128.0 - 64.0 + jnp.arange(256, dtype=jnp.float32)
        across = jnp.maximum(0.0, 1.0 - jnp.abs(along_x[:, None] - col_pos[None, :])).astype(jnp.bfloat16)
        mixed_rows = jnp.dot(across.astype(jnp.float32), jnp.transpose(window.astype(jnp.float32)), precision=PRECISE)
        tent_y = jnp.maximum(0.0, 1.0 - jnp.abs(along_y[:, None] - row_pos[None, :])) * slot_live
        return jnp.sum(mixed_rows * tent_y, axis=1)

    pieces = lax.map(one_block, (block_y, block_x, windows, block_ids))
    return pieces.reshape(block_count, H, 128).transpose(1, 0, 2).reshape(H, W).astype(jnp.bfloat16)


def reference(points, source, slab_first, slab_count):
    strip_ids = jnp.arange(N_TY, dtype=jnp.int32)
    padded_pts = jnp.pad(points, ((0, 0), (P_SIZE, P_SIZE)))
    vertex_x, vertex_y = vertex_frame()

    def fit_strip(strip_id):
        nearby = lax.dynamic_slice_in_dim(padded_pts, strip_id * P_SIZE, 3 * P_SIZE, 1)
        owners = strip_id - 1 + jnp.arange(3 * P_SIZE, dtype=jnp.int32) // P_SIZE
        usable = ((owners >= 0) & (owners < N_TY)).astype(jnp.float32)
        return solve_affine(block_moments(nearby, usable, strip_id), vertex_x, vertex_y)

    affines = lax.map(fit_strip, strip_ids)
    vertex_affines = jnp.transpose(affines, (1, 0, 2, 3)).reshape(6, N_TY * VR, VC)
    flat_shift = vertex_affines[4:6]
    extended = jnp.concatenate([flat_shift[:, :1], flat_shift, flat_shift[:, -1:]], axis=1)
    source_pad = jnp.pad(source, ((0, K * BH), (0, 0)))
    tent_rows, tent_cols = tent_tables()

    def render_one(strip_id):
        near_shift = lax.dynamic_slice_in_dim(extended, strip_id * VR, VR + 2, 1)
        disp = displace(near_shift, tent_rows, tent_cols)
        first_slab = slab_first[strip_id]
        slab_total = slab_count[strip_id]
        slab_rows = lax.dynamic_slice_in_dim(source_pad, (first_slab * BH).astype(jnp.int32), K * BH, 0)
        return render_strip(slab_rows, first_slab, slab_total, disp, strip_id)

    rendered = lax.map(render_one, strip_ids).reshape(N_TY * H, W)
    return rendered, vertex_affines
```

```python
import jax
import jax.numpy as jnp
from jax import lax
from jax.experimental import pallas as pl
from jax.experimental.pallas import tpu as pltpu
from jax.sharding import PartitionSpec as P

W = 2048
BH = 16
PC = 4
SP = 8
H = 32
K = 6
VR = 4
VC = 256


PRECISE = lax.Precision.HIGHEST
RIDGE_TERM = 0.01


def with_halo(block, sides, width):
    for axis, dim in sides:
        count = lax.axis_size(axis)
        forward = [(i, i + 1) for i in range(count - 1)]
        backward = [(target, source) for source, target in forward]
        low = lax.ppermute(
            lax.slice_in_dim(block, block.shape[dim] - width, None, axis=dim), axis, forward
        )
        high = lax.ppermute(lax.slice_in_dim(block, 0, width, axis=dim), axis, backward)
        block = jnp.concatenate([low, block, high], axis=dim)
    return block


def solve_affine(moments, vertex_x, vertex_y):
    mass = moments[0]
    mean_px = moments[1] / mass
    mean_py = moments[2] / mass
    mean_qx = moments[3] / mass
    mean_qy = moments[4] / mass
    cov_xx = moments[5] / mass - mean_px * mean_px + RIDGE_TERM
    cov_xy = moments[6] / mass - mean_px * mean_py
    cov_yy = moments[7] / mass - mean_py * mean_py + RIDGE_TERM
    cross_xx = moments[8] / mass - mean_qx * mean_px
    cross_xy = moments[9] / mass - mean_qx * mean_py
    cross_yx = moments[10] / mass - mean_qy * mean_px
    cross_yy = moments[11] / mass - mean_qy * mean_py
    determ = cov_xx * cov_yy - cov_xy * cov_xy
    lin_xx = (cross_xx * cov_yy - cross_xy * cov_xy) / determ
    lin_xy = (cross_xy * cov_xx - cross_xx * cov_xy) / determ
    lin_yx = (cross_yx * cov_yy - cross_yy * cov_xy) / determ
    lin_yy = (cross_yy * cov_xx - cross_yx * cov_xy) / determ
    delta_x = vertex_x - mean_px
    delta_y = vertex_y - mean_py
    shift_x = mean_qx + lin_xx * delta_x + lin_xy * delta_y - vertex_x
    shift_y = mean_qy + lin_yx * delta_x + lin_yy * delta_y - vertex_y
    return jnp.stack([lin_xx, lin_xy, lin_yx, lin_yy, shift_x, shift_y])


def block_moments(pts, usable, strip_id):
    block_count = W // 128
    per_block = VC // block_count
    cell_rows = pts.shape[1] // (block_count * 8 * PC)
    grid = pts.reshape(4, cell_rows, block_count, 8 * PC)
    live = usable.reshape(cell_rows, block_count, 8 * PC)
    grid = jnp.pad(grid, ((0, 0), (0, 0), (1, 1), (0, 0)))
    live = jnp.pad(live, ((0, 0), (1, 1), (0, 0)))
    near = jnp.concatenate(
        [
            grid[:, :, 0:block_count],
            grid[:, :, 1 : block_count + 1],
            grid[:, :, 2 : block_count + 2],
        ],
        axis=3,
    )
    near_live = jnp.concatenate(
        [live[:, 0:block_count], live[:, 1 : block_count + 1], live[:, 2 : block_count + 2]], axis=2
    )
    near = jnp.transpose(near, (0, 2, 1, 3)).reshape(4, block_count, cell_rows * 24 * PC)
    near_live = jnp.transpose(near_live, (1, 0, 2)).reshape(block_count, cell_rows * 24 * PC)
    centre_y = strip_id.astype(jnp.float32) * H + H / 2.0
    anchor = jnp.arange(block_count, dtype=jnp.float32) * 128.0 + 64.0
    fixed_x = (near[0] - anchor[:, None]) / H
    fixed_y = (near[1] - centre_y) / H
    moved_x = (near[2] - anchor[:, None]) / H
    moved_y = (near[3] - centre_y) / H
    unit_row = jnp.ones_like(fixed_x)
    features = (
        jnp.stack(
            [
                unit_row,
                fixed_x,
                fixed_y,
                moved_x,
                moved_y,
                fixed_x * fixed_x,
                fixed_x * fixed_y,
                fixed_y * fixed_y,
                moved_x * fixed_x,
                moved_x * fixed_y,
                moved_y * fixed_x,
                moved_y * fixed_y,
            ],
            axis=1,
        )
        * near_live[:, None, :]
    )
    vertex_col = jnp.arange(VC, dtype=jnp.float32).reshape(block_count, per_block) * SP + SP / 2.0
    vertex_row = jnp.arange(VR, dtype=jnp.float32) * SP + SP / 2.0 - H / 2.0
    gap_x = (near[0][:, :, None] - vertex_col[:, None, :]) / H
    gap_y = fixed_y[:, :, None] - (vertex_row / H)[None, None, :]
    weight_x = jnp.exp(-2.0 * gap_x * gap_x)
    weight_y = jnp.exp(-2.0 * gap_y * gap_y)
    weighted = features[:, :, None, :] * jnp.transpose(weight_y, (0, 2, 1))[:, None, :, :]
    moments = jnp.einsum("bkrm,bmc->bkrc", weighted, weight_x, precision=PRECISE)
    return jnp.transpose(moments, (1, 2, 0, 3)).reshape(12, VR, VC)


def vertex_frame():
    block_count = W // 128
    per_block = VC // block_count
    anchor = jnp.arange(block_count, dtype=jnp.float32) * 128.0 + 64.0
    vertex_col = jnp.arange(VC, dtype=jnp.float32) * SP + SP / 2.0
    vertex_row = jnp.arange(VR, dtype=jnp.float32) * SP + SP / 2.0 - H / 2.0
    column_anchor = jnp.repeat(anchor, per_block)
    vertex_x = jnp.broadcast_to(((vertex_col - column_anchor) / H)[None, :], (VR, VC))
    vertex_y = jnp.broadcast_to((vertex_row / H)[:, None], (VR, VC))
    return (vertex_x, vertex_y)


GROUP = 16
GUARD = 40
ROWS_HELD = 144


def split3(x):
    a = x.astype(jnp.bfloat16)
    r = x - a.astype(jnp.float32)
    b = r.astype(jnp.bfloat16)
    c = (r - b.astype(jnp.float32)).astype(jnp.bfloat16)
    return a, b, c


def render_kernel(first_ref, count_ref, shift_ref, src_ref, out_ref,
                  img, fine, sy_s, ix_s, w0_s, w1_s, low_v, num_v, low_m, num_m, sems):
    blocks = W // 128
    tile = lax.axis_index("ty")
    f32 = jnp.float32
    u = shift_ref[...].reshape(16, VC)
    stacked = jnp.concatenate([p.astype(f32) for p in split3(u)], axis=0).astype(jnp.bfloat16)
    for part in range(W // 256):
        col = lax.broadcasted_iota(jnp.int32, (VC, 256), 1) + part * 256
        col = jnp.clip(col, SP // 2, W - SP // 2)
        ver = lax.broadcasted_iota(jnp.int32, (VC, 256), 0) * SP + SP // 2
        tent = jnp.maximum(0.0, 1.0 - jnp.abs(col - ver).astype(f32) * (1.0 / SP)).astype(jnp.bfloat16)
        got = jnp.dot(stacked, tent, preferred_element_type=f32)
        got = got[0:16] + got[16:32] + got[32:48]
        fine[2 * part] = got[:, :128]
        fine[2 * part + 1] = got[:, 128:]

    first = first_ref[0] * BH - tile * H + H
    last = first + count_ref[0] * BH
    rows = lax.broadcasted_iota(jnp.int32, (3 * H, 128), 0)
    live = (rows >= first) & (rows < last)
    left = lax.broadcasted_iota(jnp.int32, (3 * H, 128), 1) < 64
    zero = jnp.zeros((3 * H, 128), f32)
    prev = zero
    lead = GUARD - H
    for k in range(blocks + 1):
        if k < blocks:
            now = pltpu.roll(jnp.where(live, src_ref[:, 128 * k : 128 * k + 128].astype(f32), 0.0), 64, 1)
        else:
            now = zero
        img[k, 0:lead, :] = jnp.zeros((lead, 128), f32)
        img[k, lead : lead + 3 * H, :] = jnp.where(left, prev, now)
        img[k, lead + 3 * H :, :] = jnp.zeros((ROWS_HELD - lead - 3 * H, 128), f32)
        prev = now

    sub = lax.broadcasted_iota(jnp.int32, (8, 128), 0)
    subf = sub.astype(f32)
    lane = lax.broadcasted_iota(jnp.int32, (8, 128), 1)
    wa = jnp.maximum(0.0, 1.0 - (subf + 4.0) * (1.0 / SP))
    wb = jnp.maximum(0.0, 1.0 - jnp.abs(subf - 4.0) * (1.0 / SP))
    wc = jnp.maximum(0.0, 1.0 - (12.0 - subf) * (1.0 / SP))
    lanef = lane.astype(f32)

    def prepare(b, carry):
        lows, highs = carry
        f = fine[b]
        new_lows, new_highs = [], []
        for g in range(VR):
            dx = wa * f[g : g + 1] + wb * f[g + 1 : g + 2] + wc * f[g + 2 : g + 3]
            dy = wa * f[g + 8 : g + 9] + wb * f[g + 9 : g + 10] + wc * f[g + 10 : g + 11]
            sy = jnp.clip(subf + (8.0 * g) + H * dy, -33.0, 64.0)
            sx = (lanef + (b * 128).astype(f32)) + H * dx
            lx = jnp.clip(sx - (b * 128 - 64).astype(f32), -1.0, 256.0)
            base = jnp.floor(lx)
            frac = lx - base
            ix = base.astype(jnp.int32)
            w0 = jnp.where((ix >= 0) & (ix < 256), 1.0 - frac, 0.0).astype(jnp.bfloat16).astype(f32)
            w1 = jnp.where(ix < 255, frac, 0.0).astype(jnp.bfloat16).astype(f32)
            r = slice(8 * g, 8 * g + 8)
            sy_s[b, r, :] = sy
            ix_s[b, r, :] = ix
            w0_s[b, r, :] = w0
            w1_s[b, r, :] = w1
            lo = jnp.min(sy, axis=1, keepdims=True)
            hi = jnp.max(sy, axis=1, keepdims=True)
            new_lows.append(jnp.where(lane == b, lo, lows[g]))
            new_highs.append(jnp.where(lane == b, hi, highs[g]))
        return tuple(new_lows), tuple(new_highs)

    start = tuple(jnp.zeros((8, 128), f32) for _ in range(VR))
    lows, highs = lax.fori_loop(0, blocks, prepare, (start, start))
    low = jnp.floor(jnp.concatenate(lows, axis=0)).astype(jnp.int32)
    high = jnp.floor(jnp.concatenate(highs, axis=0)).astype(jnp.int32)
    low_v[...] = low
    chunks = (high + 1 - low) // 8 + 1
    num_v[...] = jnp.concatenate(
        [jnp.broadcast_to(jnp.max(chunks[GROUP * i : GROUP * (i + 1)], axis=0, keepdims=True), (8, 128))
         for i in range(H // GROUP)], axis=0)
    c1 = pltpu.make_async_copy(low_v, low_m, sems.at[0])
    c2 = pltpu.make_async_copy(num_v, num_m, sems.at[1])
    c1.start()
    c2.start()
    c1.wait()
    c2.wait()

    def paint(b, _):
        for q in range(H // GROUP):
            def chunk(k, accs):
                res = []
                for j in range(GROUP):
                    r = q * GROUP + j
                    base = low_m[r, b] + 8 * k
                    at = jnp.minimum(base + GUARD, ROWS_HELD - 8)
                    s0 = img[b, pl.ds(at, 8), :]
                    s1 = img[b + 1, pl.ds(at, 8), :]
                    i0 = jnp.broadcast_to(ix_s[b, r : r + 1, :], (8, 128))
                    i1 = i0 + 1
                    m0 = i0 & 127
                    m1 = i1 & 127
                    g0 = jnp.where(i0 < 128, jnp.take_along_axis(s0, m0, axis=1), jnp.take_along_axis(s1, m0, axis=1))
                    g1 = jnp.where(i1 < 128, jnp.take_along_axis(s0, m1, axis=1), jnp.take_along_axis(s1, m1, axis=1))
                    mixed = g0 * w0_s[b, r : r + 1, :] + g1 * w1_s[b, r : r + 1, :]
                    ty = jnp.maximum(0.0, 1.0 - jnp.abs((sy_s[b, r : r + 1, :] - base.astype(f32)) - subf))
                    res.append(accs[j] + mixed * ty)
                return tuple(res)

            accs = lax.fori_loop(0, num_m[8 * q, b], chunk, tuple(jnp.zeros((8, 128), f32) for _ in range(GROUP)))
            rows_out = jnp.concatenate([jnp.sum(a, axis=0, keepdims=True) for a in accs], axis=0)
            out_ref[q * GROUP : (q + 1) * GROUP, pl.ds(pl.multiple_of(b * 128, 128), 128)] = rows_out.astype(jnp.bfloat16)
        return 0

    lax.fori_loop(0, blocks, paint, 0)


def render(first, count, shift, src):
    blocks = W // 128
    vm = pl.BlockSpec(memory_space=pltpu.VMEM)
    sm = pl.BlockSpec(memory_space=pltpu.SMEM)
    per = lambda d: pltpu.VMEM((blocks, H, 128), d)
    return pl.pallas_call(
        render_kernel,
        out_shape=jax.ShapeDtypeStruct((H, W), jnp.bfloat16),
        in_specs=[sm, sm, vm, vm],
        out_specs=vm,
        scratch_shapes=[
            pltpu.VMEM((blocks + 1, ROWS_HELD, 128), jnp.float32),
            pltpu.VMEM((blocks, 16, 128), jnp.float32),
            per(jnp.float32), per(jnp.int32), per(jnp.float32), per(jnp.float32),
            pltpu.VMEM((H, 128), jnp.int32),
            pltpu.VMEM((8 * (H // GROUP), 128), jnp.int32),
            pltpu.SMEM((H, 128), jnp.int32),
            pltpu.SMEM((8 * (H // GROUP), 128), jnp.int32),
            pltpu.SemaphoreType.DMA((2,)),
        ],
        name="render",
    )(first, count, shift, src)


def per_device(points, source, slab_first, slab_count):
    strip_id = lax.axis_index("ty")
    strip_span = lax.axis_size("ty")
    tile_len = points.shape[1]
    vertex_x, vertex_y = vertex_frame()
    nearby = with_halo(points, (("ty", 1),), tile_len)
    owners = strip_id - 1 + jnp.arange(3 * tile_len, dtype=jnp.int32) // tile_len
    usable = ((owners >= 0) & (owners < strip_span)).astype(jnp.float32)
    moments = block_moments(nearby, usable, strip_id)
    affines = solve_affine(moments, vertex_x, vertex_y)
    own_shift = affines[4:6]
    extended = with_halo(own_shift, (("ty", 1),), 1)
    upper_row = jnp.where(strip_id == 0, own_shift[:, :1], extended[:, :1])
    lower_row = jnp.where(strip_id == strip_span - 1, own_shift[:, -1:], extended[:, -1:])
    near_shift = jnp.concatenate([upper_row, own_shift, lower_row], axis=1)
    wider = with_halo(source, (("ty", 0),), H)
    near_shift = jnp.pad(near_shift, ((0, 0), (0, 2), (0, 0)))
    rendered = render(slab_first, slab_count, near_shift, wider)
    return (rendered, affines)


def solution(mesh):
    return jax.shard_map(
        per_device,
        mesh=mesh,
        in_specs=(
            P(None, ("sec", "ty")),
            P(("sec", "ty"), None),
            P(("sec", "ty")),
            P(("sec", "ty")),
        ),
        out_specs=(P(("sec", "ty"), None), P(None, ("sec", "ty"), None)),
        check_vma=False,
    )
```

```python
import jax
import jax.numpy as jnp
from jax import lax
from jax.experimental import pallas as pl
from jax.experimental.pallas import tpu as pltpu
from jax.sharding import PartitionSpec as P

W = 2048
BH = 16
SP = 8
H = 32
K = 6
VR = 4
VC = 256


MESH = pl.DeviceIdType.MESH
RIDGE_TERM = 0.01


def solve_affine(moments, vertex_x, vertex_y):
    mass = moments[0]
    mean_px = moments[1] / mass
    mean_py = moments[2] / mass
    mean_qx = moments[3] / mass
    mean_qy = moments[4] / mass
    cov_xx = moments[5] / mass - mean_px * mean_px + RIDGE_TERM
    cov_xy = moments[6] / mass - mean_px * mean_py
    cov_yy = moments[7] / mass - mean_py * mean_py + RIDGE_TERM
    cross_xx = moments[8] / mass - mean_qx * mean_px
    cross_xy = moments[9] / mass - mean_qx * mean_py
    cross_yx = moments[10] / mass - mean_qy * mean_px
    cross_yy = moments[11] / mass - mean_qy * mean_py
    determ = cov_xx * cov_yy - cov_xy * cov_xy
    lin_xx = (cross_xx * cov_yy - cross_xy * cov_xy) / determ
    lin_xy = (cross_xy * cov_xx - cross_xx * cov_xy) / determ
    lin_yx = (cross_yx * cov_yy - cross_yy * cov_xy) / determ
    lin_yy = (cross_yy * cov_xx - cross_yx * cov_xy) / determ
    delta_x = vertex_x - mean_px
    delta_y = vertex_y - mean_py
    shift_x = mean_qx + lin_xx * delta_x + lin_xy * delta_y - vertex_x
    shift_y = mean_qy + lin_yx * delta_x + lin_yy * delta_y - vertex_y
    return [lin_xx, lin_xy, lin_yx, lin_yy, shift_x, shift_y]


OFFSETS = (1, -1, 2, -2)


def fit_kernel(pts_ref, src_ref, fit_ref, slab_ref,
               held, wide, staged, mom, send_p, recv_p, send_s, recv_s):
    f32 = jnp.float32
    me = lax.axis_index("ty")
    n = lax.axis_size("ty")
    size = pts_ref.shape[1]
    half = size // 2
    pairs = W // 256

    def exists(d):
        return (me + d >= 0) & (me + d < n)

    barrier = pltpu.get_barrier_semaphore()
    for d in OFFSETS:
        @pl.when(exists(d))
        def _(d=d):
            pl.semaphore_signal(barrier, inc=1, device_id={"ty": me + d}, device_id_type=MESH)
    peers = sum(exists(d).astype(jnp.int32) for d in OFFSETS)
    pl.semaphore_wait(barrier, peers)

    def points_to(i, d):
        return pltpu.make_async_remote_copy(
            src_ref=pts_ref, dst_ref=held.at[2 - d], send_sem=send_p.at[i], recv_sem=recv_p.at[i],
            device_id={"ty": me + d}, device_id_type=MESH)

    def source_to(i, d):
        return pltpu.make_async_remote_copy(
            src_ref=src_ref, dst_ref=wide.at[i], send_sem=send_s.at[i], recv_sem=recv_s.at[i],
            device_id={"ty": me + d}, device_id_type=MESH)

    for i, d in enumerate(OFFSETS):
        @pl.when(exists(d))
        def _(i=i, d=d):
            points_to(i, d).start()
    for i, d in enumerate(OFFSETS[:2]):
        @pl.when(exists(d))
        def _(i=i, d=d):
            source_to(i, d).start()
    slab_ref[H : 2 * H, :] = src_ref[...]
    for i, d in enumerate(OFFSETS):
        @pl.when(exists(-d))
        def _(i=i, d=d):
            points_to(i, d).wait_recv()

    spare = jnp.zeros((4, 128), f32)
    for tile in range(5):
        data = pts_ref[...] if tile == 2 else jnp.where(exists(tile - 2), held[tile], 0.0)
        for c in range(2):
            row = jnp.concatenate([data[:, c * half : (c + 1) * half], spare], axis=1)
            staged[0, 2 * tile + c] = pltpu.roll(row, 32, 1)
            staged[1, 2 * tile + c] = pltpu.roll(row, half + 96, 1)

    e = lax.broadcasted_iota(jnp.int32, (8, 128), 0)
    own = jnp.where(e == 0, 1, jnp.where(e == 5, 3, 2))
    vy = (((e - 1) * SP + SP // 2) - H // 2).astype(f32) * (1.0 / H)
    lane32 = lax.broadcasted_iota(jnp.int32, (32, 128), 1)
    vert32 = lax.broadcasted_iota(jnp.int32, (32, 128), 0)
    vx32 = (vert32 * SP + SP // 2 - 128).astype(f32) * (1.0 / H)
    centre = (me * H).astype(f32) + H / 2.0

    def group(k, _):
        for odd in range(2):
            pair = 2 * k + odd
            anchor = (pair * 256 + 128).astype(f32)
            block = 2 * pair - 1 + lane32 // 32
            mine = 2 * pair + vert32 // 16
            near = (jnp.abs(block - mine) <= 1) & (block >= 0) & (block < 2 * pairs)
            parts, weights = [], []
            for t in range(10):
                tile = t // 2
                box = staged[odd, t, :, pl.ds(pl.multiple_of(k * 128, 128), 128)]
                px = (box[0:1] - anchor) * (1.0 / H)
                py = (box[1:2] - centre) * (1.0 / H)
                qx = (box[2:3] - anchor) * (1.0 / H)
                qy = (box[3:4] - centre) * (1.0 / H)
                gap = px - vx32
                across = jnp.where(near, jnp.exp(-2.0 * gap * gap), 0.0)
                near_part = across.astype(jnp.bfloat16)
                rest_part = (across - near_part.astype(f32)).astype(jnp.bfloat16)
                weights.append(jnp.concatenate([near_part, rest_part], axis=0))
                rise = py - vy
                there = (jnp.abs(own - tile) <= 1) & exists(tile - 2)
                w = jnp.where(there, jnp.exp(-2.0 * rise * rise), 0.0)
                wpx = w * px
                wpy = w * py
                feats = jnp.concatenate(
                    [w, wpx, wpy, w * qx, w * qy, wpx * px, wpx * py, wpy * py,
                     wpx * qx, wpy * qx, wpx * qy, wpy * qy], axis=0)
                high = feats.astype(jnp.bfloat16)
                low = (feats - high.astype(f32)).astype(jnp.bfloat16)
                parts.append(jnp.concatenate([high, low], axis=0))
            got = lax.dot_general(
                jnp.concatenate(parts, axis=1), jnp.concatenate(weights, axis=1),
                (((1,), (1,)), ((), ())), preferred_element_type=f32)
            got = got[0:96] + got[96:192]
            mom[pair] = got[:, 0:32] + got[:, 32:64]
        return 0

    lax.fori_loop(0, pairs // 2, group, 0)
    moments = [
        jnp.concatenate([mom[g, 8 * f : 8 * f + 8, :] for g in range(pairs)], axis=1) for f in range(12)
    ]
    ew = lax.broadcasted_iota(jnp.int32, (8, VC), 0)
    jw = lax.broadcasted_iota(jnp.int32, (8, VC), 1)
    vertex_y = (((ew - 1) * SP + SP // 2) - H // 2).astype(f32) * (1.0 / H)
    vertex_x = ((jw % 32) * SP + SP // 2 - 128).astype(f32) * (1.0 / H)
    safe = ew < 6
    moments[0] = jnp.where(safe, moments[0], 1.0)
    solved = solve_affine(moments, vertex_x, vertex_y)
    for f in range(6):
        x = solved[f]
        if f >= 4:
            x = jnp.where((ew == 0) & (me == 0), x[1:2], x)
            x = jnp.where((ew == 5) & (me == n - 1), x[4:5], x)
            x = jnp.where(safe, x, 0.0)
        fit_ref[8 * f : 8 * f + 8, :] = x

    for i, d in enumerate(OFFSETS[:2]):
        @pl.when(exists(-d))
        def _(i=i, d=d):
            source_to(i, d).wait_recv()
    slab_ref[0:H, :] = wide[0]
    slab_ref[2 * H :, :] = wide[1]
    for i, d in enumerate(OFFSETS):
        @pl.when(exists(d))
        def _(i=i, d=d):
            points_to(i, d).wait_send()
    for i, d in enumerate(OFFSETS[:2]):
        @pl.when(exists(d))
        def _(i=i, d=d):
            source_to(i, d).wait_send()


def fit(points, source):
    size = points.shape[1]
    vm = pl.BlockSpec(memory_space=pltpu.VMEM)
    return pl.pallas_call(
        fit_kernel,
        out_shape=(
            jax.ShapeDtypeStruct((48, VC), jnp.float32),
            jax.ShapeDtypeStruct((3 * H, W), jnp.bfloat16),
        ),
        in_specs=[vm, vm],
        out_specs=(vm, vm),
        scratch_shapes=[
            pltpu.VMEM((5, 4, size), jnp.float32),
            pltpu.VMEM((2, H, W), jnp.bfloat16),
            pltpu.VMEM((2, 10, 4, size // 2 + 128), jnp.float32),
            pltpu.VMEM((W // 256, 96, 32), jnp.float32),
            pltpu.SemaphoreType.DMA((4,)),
            pltpu.SemaphoreType.DMA((4,)),
            pltpu.SemaphoreType.DMA((2,)),
            pltpu.SemaphoreType.DMA((2,)),
        ],
        compiler_params=pltpu.CompilerParams(collective_id=0, has_side_effects=True),
        name="fit",
    )(points, source)


GROUP = 16
GUARD = 40
ROWS_HELD = 144


def split3(x):
    a = x.astype(jnp.bfloat16)
    r = x - a.astype(jnp.float32)
    b = r.astype(jnp.bfloat16)
    c = (r - b.astype(jnp.float32)).astype(jnp.bfloat16)
    return a, b, c


def render_kernel(first_ref, count_ref, fit_ref, src_ref, out_ref, aff_ref,
                  img, fine, sy_s, ix_s, w0_s, w1_s, low_v, num_v, low_m, num_m, sems):
    blocks = W // 128
    tile = lax.axis_index("ty")
    f32 = jnp.float32
    for f in range(6):
        aff_ref[f] = fit_ref[8 * f + 1 : 8 * f + 5, :]
    u = fit_ref[32:48, :]
    stacked = jnp.concatenate([p.astype(f32) for p in split3(u)], axis=0).astype(jnp.bfloat16)
    for part in range(W // 256):
        col = lax.broadcasted_iota(jnp.int32, (VC, 256), 1) + part * 256
        col = jnp.clip(col, SP // 2, W - SP // 2)
        ver = lax.broadcasted_iota(jnp.int32, (VC, 256), 0) * SP + SP // 2
        tent = jnp.maximum(0.0, 1.0 - jnp.abs(col - ver).astype(f32) * (1.0 / SP)).astype(jnp.bfloat16)
        got = jnp.dot(stacked, tent, preferred_element_type=f32)
        got = got[0:16] + got[16:32] + got[32:48]
        fine[2 * part] = got[:, :128]
        fine[2 * part + 1] = got[:, 128:]

    first = first_ref[0] * BH - tile * H + H
    last = first + count_ref[0] * BH
    rows = lax.broadcasted_iota(jnp.int32, (3 * H, 128), 0)
    live = (rows >= first) & (rows < last)
    left = lax.broadcasted_iota(jnp.int32, (3 * H, 128), 1) < 64
    zero = jnp.zeros((3 * H, 128), f32)
    prev = zero
    lead = GUARD - H
    for k in range(blocks + 1):
        if k < blocks:
            now = pltpu.roll(jnp.where(live, src_ref[:, 128 * k : 128 * k + 128].astype(f32), 0.0), 64, 1)
        else:
            now = zero
        img[k, 0:lead, :] = jnp.zeros((lead, 128), f32)
        img[k, lead : lead + 3 * H, :] = jnp.where(left, prev, now)
        img[k, lead + 3 * H :, :] = jnp.zeros((ROWS_HELD - lead - 3 * H, 128), f32)
        prev = now

    sub = lax.broadcasted_iota(jnp.int32, (8, 128), 0)
    subf = sub.astype(f32)
    lane = lax.broadcasted_iota(jnp.int32, (8, 128), 1)
    wa = jnp.maximum(0.0, 1.0 - (subf + 4.0) * (1.0 / SP))
    wb = jnp.maximum(0.0, 1.0 - jnp.abs(subf - 4.0) * (1.0 / SP))
    wc = jnp.maximum(0.0, 1.0 - (12.0 - subf) * (1.0 / SP))
    lanef = lane.astype(f32)

    def prepare(b, carry):
        lows, highs = carry
        f = fine[b]
        new_lows, new_highs = [], []
        for g in range(VR):
            dx = wa * f[g : g + 1] + wb * f[g + 1 : g + 2] + wc * f[g + 2 : g + 3]
            dy = wa * f[g + 8 : g + 9] + wb * f[g + 9 : g + 10] + wc * f[g + 10 : g + 11]
            sy = jnp.clip(subf + (8.0 * g) + H * dy, -33.0, 64.0)
            sx = (lanef + (b * 128).astype(f32)) + H * dx
            lx = jnp.clip(sx - (b * 128 - 64).astype(f32), -1.0, 256.0)
            base = jnp.floor(lx)
            frac = lx - base
            ix = base.astype(jnp.int32)
            w0 = jnp.where((ix >= 0) & (ix < 256), 1.0 - frac, 0.0).astype(jnp.bfloat16).astype(f32)
            w1 = jnp.where(ix < 255, frac, 0.0).astype(jnp.bfloat16).astype(f32)
            r = slice(8 * g, 8 * g + 8)
            sy_s[b, r, :] = sy
            ix_s[b, r, :] = ix
            w0_s[b, r, :] = w0
            w1_s[b, r, :] = w1
            lo = jnp.min(sy, axis=1, keepdims=True)
            hi = jnp.max(sy, axis=1, keepdims=True)
            new_lows.append(jnp.where(lane == b, lo, lows[g]))
            new_highs.append(jnp.where(lane == b, hi, highs[g]))
        return tuple(new_lows), tuple(new_highs)

    start = tuple(jnp.zeros((8, 128), f32) for _ in range(VR))
    lows, highs = lax.fori_loop(0, blocks, prepare, (start, start))
    low = jnp.floor(jnp.concatenate(lows, axis=0)).astype(jnp.int32)
    high = jnp.floor(jnp.concatenate(highs, axis=0)).astype(jnp.int32)
    low_v[...] = low
    chunks = (high + 1 - low) // 8 + 1
    num_v[...] = jnp.concatenate(
        [jnp.broadcast_to(jnp.max(chunks[GROUP * i : GROUP * (i + 1)], axis=0, keepdims=True), (8, 128))
         for i in range(H // GROUP)], axis=0)
    c1 = pltpu.make_async_copy(low_v, low_m, sems.at[0])
    c2 = pltpu.make_async_copy(num_v, num_m, sems.at[1])
    c1.start()
    c2.start()
    c1.wait()
    c2.wait()

    def paint(b, _):
        for q in range(H // GROUP):
            def chunk(k, accs):
                res = []
                for j in range(GROUP):
                    r = q * GROUP + j
                    base = low_m[r, b] + 8 * k
                    at = jnp.minimum(base + GUARD, ROWS_HELD - 8)
                    s0 = img[b, pl.ds(at, 8), :]
                    s1 = img[b + 1, pl.ds(at, 8), :]
                    i0 = jnp.broadcast_to(ix_s[b, r : r + 1, :], (8, 128))
                    i1 = i0 + 1
                    m0 = i0 & 127
                    m1 = i1 & 127
                    g0 = jnp.where(i0 < 128, jnp.take_along_axis(s0, m0, axis=1), jnp.take_along_axis(s1, m0, axis=1))
                    g1 = jnp.where(i1 < 128, jnp.take_along_axis(s0, m1, axis=1), jnp.take_along_axis(s1, m1, axis=1))
                    mixed = g0 * w0_s[b, r : r + 1, :] + g1 * w1_s[b, r : r + 1, :]
                    ty = jnp.maximum(0.0, 1.0 - jnp.abs((sy_s[b, r : r + 1, :] - base.astype(f32)) - subf))
                    res.append(accs[j] + mixed * ty)
                return tuple(res)

            accs = lax.fori_loop(0, num_m[8 * q, b], chunk, tuple(jnp.zeros((8, 128), f32) for _ in range(GROUP)))
            rows_out = jnp.concatenate([jnp.sum(a, axis=0, keepdims=True) for a in accs], axis=0)
            out_ref[q * GROUP : (q + 1) * GROUP, pl.ds(pl.multiple_of(b * 128, 128), 128)] = rows_out.astype(jnp.bfloat16)
        return 0

    lax.fori_loop(0, blocks, paint, 0)


def render(first, count, shift, src):
    blocks = W // 128
    vm = pl.BlockSpec(memory_space=pltpu.VMEM)
    sm = pl.BlockSpec(memory_space=pltpu.SMEM)
    per = lambda d: pltpu.VMEM((blocks, H, 128), d)
    return pl.pallas_call(
        render_kernel,
        out_shape=(
            jax.ShapeDtypeStruct((H, W), jnp.bfloat16),
            jax.ShapeDtypeStruct((6, VR, VC), jnp.float32),
        ),
        in_specs=[sm, sm, vm, vm],
        out_specs=(vm, vm),
        scratch_shapes=[
            pltpu.VMEM((blocks + 1, ROWS_HELD, 128), jnp.float32),
            pltpu.VMEM((blocks, 16, 128), jnp.float32),
            per(jnp.float32), per(jnp.int32), per(jnp.float32), per(jnp.float32),
            pltpu.VMEM((H, 128), jnp.int32),
            pltpu.VMEM((8 * (H // GROUP), 128), jnp.int32),
            pltpu.SMEM((H, 128), jnp.int32),
            pltpu.SMEM((8 * (H // GROUP), 128), jnp.int32),
            pltpu.SemaphoreType.DMA((2,)),
        ],
        name="render",
    )(first, count, shift, src)


def per_device(points, source, slab_first, slab_count):
    fitted, slab = fit(points, source)
    rendered, affines = render(slab_first, slab_count, fitted, slab)
    return (rendered, affines)


def solution(mesh):
    return jax.shard_map(
        per_device,
        mesh=mesh,
        in_specs=(
            P(None, ("sec", "ty")),
            P(("sec", "ty"), None),
            P(("sec", "ty")),
            P(("sec", "ty")),
        ),
        out_specs=(P(("sec", "ty"), None), P(None, ("sec", "ty"), None)),
        check_vma=False,
    )
```

```python
import jax
import jax.numpy as jnp
from jax import lax
from jax.experimental import pallas as pl
from jax.experimental.pallas import tpu as pltpu
from jax.sharding import PartitionSpec as P

W = 2048
BH = 16
SP = 8
H = 32
K = 6
VR = 4
VC = 256


MESH = pl.DeviceIdType.MESH
RIDGE_TERM = 0.01


def solve_affine(moments, vertex_x, vertex_y):
    mass = moments[0]
    mean_px = moments[1] / mass
    mean_py = moments[2] / mass
    mean_qx = moments[3] / mass
    mean_qy = moments[4] / mass
    cov_xx = moments[5] / mass - mean_px * mean_px + RIDGE_TERM
    cov_xy = moments[6] / mass - mean_px * mean_py
    cov_yy = moments[7] / mass - mean_py * mean_py + RIDGE_TERM
    cross_xx = moments[8] / mass - mean_qx * mean_px
    cross_xy = moments[9] / mass - mean_qx * mean_py
    cross_yx = moments[10] / mass - mean_qy * mean_px
    cross_yy = moments[11] / mass - mean_qy * mean_py
    determ = cov_xx * cov_yy - cov_xy * cov_xy
    lin_xx = (cross_xx * cov_yy - cross_xy * cov_xy) / determ
    lin_xy = (cross_xy * cov_xx - cross_xx * cov_xy) / determ
    lin_yx = (cross_yx * cov_yy - cross_yy * cov_xy) / determ
    lin_yy = (cross_yy * cov_xx - cross_yx * cov_xy) / determ
    delta_x = vertex_x - mean_px
    delta_y = vertex_y - mean_py
    shift_x = mean_qx + lin_xx * delta_x + lin_xy * delta_y - vertex_x
    shift_y = mean_qy + lin_yx * delta_x + lin_yy * delta_y - vertex_y
    return [lin_xx, lin_xy, lin_yx, lin_yy, shift_x, shift_y]


OFFSETS = (1, -1, 2, -2)


def fit_kernel(pts_ref, src_ref, fit_ref, wide,
               held, staged, mom, send_p, recv_p, send_s, recv_s):
    f32 = jnp.float32
    me = lax.axis_index("ty")
    n = lax.axis_size("ty")
    size = pts_ref.shape[1]
    half = size // 2
    pairs = W // 256

    def exists(d):
        return (me + d >= 0) & (me + d < n)

    barrier = pltpu.get_barrier_semaphore()
    for d in OFFSETS:
        @pl.when(exists(d))
        def _(d=d):
            pl.semaphore_signal(barrier, inc=1, device_id={"ty": me + d}, device_id_type=MESH)
    peers = sum(exists(d).astype(jnp.int32) for d in OFFSETS)
    pl.semaphore_wait(barrier, peers)

    def points_to(i, d):
        return pltpu.make_async_remote_copy(
            src_ref=pts_ref, dst_ref=held.at[2 - d], send_sem=send_p.at[i], recv_sem=recv_p.at[i],
            device_id={"ty": me + d}, device_id_type=MESH)

    def source_to(i, d):
        return pltpu.make_async_remote_copy(
            src_ref=src_ref, dst_ref=wide.at[i], send_sem=send_s.at[i], recv_sem=recv_s.at[i],
            device_id={"ty": me + d}, device_id_type=MESH)

    for i, d in enumerate(OFFSETS):
        @pl.when(exists(d))
        def _(i=i, d=d):
            points_to(i, d).start()
    for i, d in enumerate(OFFSETS[:2]):
        @pl.when(exists(d))
        def _(i=i, d=d):
            source_to(i, d).start()
    for i, d in enumerate(OFFSETS):
        @pl.when(exists(-d))
        def _(i=i, d=d):
            points_to(i, d).wait_recv()

    spare = jnp.zeros((4, 128), f32)
    for tile in range(5):
        data = pts_ref[...] if tile == 2 else jnp.where(exists(tile - 2), held[tile], 0.0)
        for c in range(2):
            row = jnp.concatenate([data[:, c * half : (c + 1) * half], spare], axis=1)
            staged[0, 2 * tile + c] = pltpu.roll(row, 32, 1)
            staged[1, 2 * tile + c] = pltpu.roll(row, half + 96, 1)

    e = lax.broadcasted_iota(jnp.int32, (8, 128), 0)
    own = jnp.where(e == 0, 1, jnp.where(e == 5, 3, 2))
    vy = (((e - 1) * SP + SP // 2) - H // 2).astype(f32) * (1.0 / H)
    lane32 = lax.broadcasted_iota(jnp.int32, (32, 128), 1)
    vert32 = lax.broadcasted_iota(jnp.int32, (32, 128), 0)
    vx32 = (vert32 * SP + SP // 2 - 128).astype(f32) * (1.0 / H)
    centre = (me * H).astype(f32) + H / 2.0

    def group(k, _):
        for odd in range(2):
            pair = 2 * k + odd
            anchor = (pair * 256 + 128).astype(f32)
            block = 2 * pair - 1 + lane32 // 32
            mine = 2 * pair + vert32 // 16
            near = (jnp.abs(block - mine) <= 1) & (block >= 0) & (block < 2 * pairs)
            parts, weights = [], []
            for t in range(10):
                tile = t // 2
                box = staged[odd, t, :, pl.ds(pl.multiple_of(k * 128, 128), 128)]
                px = (box[0:1] - anchor) * (1.0 / H)
                py = (box[1:2] - centre) * (1.0 / H)
                qx = (box[2:3] - anchor) * (1.0 / H)
                qy = (box[3:4] - centre) * (1.0 / H)
                gap = px - vx32
                across = jnp.where(near, jnp.exp(-2.0 * gap * gap), 0.0)
                near_part = across.astype(jnp.bfloat16)
                rest_part = (across - near_part.astype(f32)).astype(jnp.bfloat16)
                weights.append(jnp.concatenate([near_part, rest_part], axis=0))
                rise = py - vy
                there = (jnp.abs(own - tile) <= 1) & exists(tile - 2)
                w = jnp.where(there, jnp.exp(-2.0 * rise * rise), 0.0)
                wpx = w * px
                wpy = w * py
                feats = jnp.concatenate(
                    [w, wpx, wpy, w * qx, w * qy, wpx * px, wpx * py, wpy * py,
                     wpx * qx, wpy * qx, wpx * qy, wpy * qy], axis=0)
                high = feats.astype(jnp.bfloat16)
                low = (feats - high.astype(f32)).astype(jnp.bfloat16)
                parts.append(jnp.concatenate([high, low], axis=0))
            got = lax.dot_general(
                jnp.concatenate(parts, axis=1), jnp.concatenate(weights, axis=1),
                (((1,), (1,)), ((), ())), preferred_element_type=f32)
            got = got[0:96] + got[96:192]
            mom[pair] = got[:, 0:32] + got[:, 32:64]
        return 0

    lax.fori_loop(0, pairs // 2, group, 0)
    moments = [
        jnp.concatenate([mom[g, 8 * f : 8 * f + 8, :] for g in range(pairs)], axis=1) for f in range(12)
    ]
    ew = lax.broadcasted_iota(jnp.int32, (8, VC), 0)
    jw = lax.broadcasted_iota(jnp.int32, (8, VC), 1)
    vertex_y = (((ew - 1) * SP + SP // 2) - H // 2).astype(f32) * (1.0 / H)
    vertex_x = ((jw % 32) * SP + SP // 2 - 128).astype(f32) * (1.0 / H)
    safe = ew < 6
    moments[0] = jnp.where(safe, moments[0], 1.0)
    solved = solve_affine(moments, vertex_x, vertex_y)
    for f in range(6):
        x = solved[f]
        if f >= 4:
            x = jnp.where((ew == 0) & (me == 0), x[1:2], x)
            x = jnp.where((ew == 5) & (me == n - 1), x[4:5], x)
            x = jnp.where(safe, x, 0.0)
        fit_ref[8 * f : 8 * f + 8, :] = x

    for i, d in enumerate(OFFSETS[:2]):
        @pl.when(exists(-d))
        def _(i=i, d=d):
            source_to(i, d).wait_recv()
    for i, d in enumerate(OFFSETS):
        @pl.when(exists(d))
        def _(i=i, d=d):
            points_to(i, d).wait_send()
    for i, d in enumerate(OFFSETS[:2]):
        @pl.when(exists(d))
        def _(i=i, d=d):
            source_to(i, d).wait_send()


def fit(points, source):
    size = points.shape[1]
    vm = pl.BlockSpec(memory_space=pltpu.VMEM)
    return pl.pallas_call(
        fit_kernel,
        out_shape=(
            jax.ShapeDtypeStruct((48, VC), jnp.float32),
            jax.ShapeDtypeStruct((2, H, W), jnp.bfloat16),
        ),
        in_specs=[vm, pl.BlockSpec(memory_space=pl.ANY)],
        out_specs=(vm, pl.BlockSpec(memory_space=pl.ANY)),
        scratch_shapes=[
            pltpu.VMEM((5, 4, size), jnp.float32),
            pltpu.VMEM((2, 10, 4, size // 2 + 128), jnp.float32),
            pltpu.VMEM((W // 256, 96, 32), jnp.float32),
            pltpu.SemaphoreType.DMA((4,)),
            pltpu.SemaphoreType.DMA((4,)),
            pltpu.SemaphoreType.DMA((2,)),
            pltpu.SemaphoreType.DMA((2,)),
        ],
        compiler_params=pltpu.CompilerParams(collective_id=0, has_side_effects=True),
        name="fit",
    )(points, source)


GUARD = 40
ROWS_HELD = 144


def split3(x):
    a = x.astype(jnp.bfloat16)
    r = x - a.astype(jnp.float32)
    b = r.astype(jnp.bfloat16)
    c = (r - b.astype(jnp.float32)).astype(jnp.bfloat16)
    return a, b, c


def render_kernel(first_ref, count_ref, fit_ref, own_ref, wide_ref, out_ref, aff_ref,
                  src_ref, img, img1, fine, rowbuf, sy_s, ix_s, w0_s, w1_s, low_v, num_v, low_m, num_m, sems):
    blocks = W // 128
    tile = lax.axis_index("ty")
    f32 = jnp.float32
    fetch = [
        pltpu.make_async_copy(own_ref, src_ref.at[pl.ds(H, H)], sems.at[2]),
        pltpu.make_async_copy(wide_ref.at[0], src_ref.at[pl.ds(0, H)], sems.at[3]),
        pltpu.make_async_copy(wide_ref.at[1], src_ref.at[pl.ds(2 * H, H)], sems.at[4]),
    ]
    for c in fetch:
        c.start()
    for f in range(6):
        aff_ref[f] = fit_ref[8 * f + 1 : 8 * f + 5, :]
    u = fit_ref[32:48, :]
    stacked = jnp.concatenate([p.astype(f32) for p in split3(u)], axis=0).astype(jnp.bfloat16)
    for part in range(W // 256):
        col = lax.broadcasted_iota(jnp.int32, (VC, 256), 1) + part * 256
        col = jnp.clip(col, SP // 2, W - SP // 2)
        ver = lax.broadcasted_iota(jnp.int32, (VC, 256), 0) * SP + SP // 2
        tent = jnp.maximum(0.0, 1.0 - jnp.abs(col - ver).astype(f32) * (1.0 / SP)).astype(jnp.bfloat16)
        got = jnp.dot(stacked, tent, preferred_element_type=f32)
        got = got[0:16] + got[16:32] + got[32:48]
        fine[2 * part] = got[:, :128]
        fine[2 * part + 1] = got[:, 128:]

    sub = lax.broadcasted_iota(jnp.int32, (8, 128), 0)
    subf = sub.astype(f32)
    lane = lax.broadcasted_iota(jnp.int32, (8, 128), 1)
    wa = jnp.maximum(0.0, 1.0 - (subf + 4.0) * (1.0 / SP))
    wb = jnp.maximum(0.0, 1.0 - jnp.abs(subf - 4.0) * (1.0 / SP))
    wc = jnp.maximum(0.0, 1.0 - (12.0 - subf) * (1.0 / SP))
    lanef = lane.astype(f32)

    def prepare(b, carry):
        lows, highs = carry
        f = fine[b]
        new_lows, new_highs = [], []
        for g in range(VR):
            dx = wa * f[g : g + 1] + wb * f[g + 1 : g + 2] + wc * f[g + 2 : g + 3]
            dy = wa * f[g + 8 : g + 9] + wb * f[g + 9 : g + 10] + wc * f[g + 10 : g + 11]
            sy = jnp.clip(subf + (8.0 * g) + H * dy, -33.0, 64.0)
            sx = (lanef + (b * 128).astype(f32)) + H * dx
            lx = jnp.clip(sx - (b * 128 - 64).astype(f32), -1.0, 256.0)
            base = jnp.floor(lx)
            frac = lx - base
            ix = base.astype(jnp.int32)
            w0 = jnp.where(ix < 0, frac, jnp.where(ix < 256, 1.0 - frac, 0.0)).astype(jnp.bfloat16).astype(f32)
            w1 = jnp.where((ix >= 0) & (ix < 255), frac, 0.0).astype(jnp.bfloat16).astype(f32)
            r = slice(8 * g, 8 * g + 8)
            sy_s[b, r, :] = sy
            ix_s[b, r, :] = jnp.clip(ix, 0, 255)
            w0_s[b, r, :] = w0
            w1_s[b, r, :] = w1
            lo = jnp.min(sy, axis=1, keepdims=True)
            hi = jnp.max(sy, axis=1, keepdims=True)
            new_lows.append(jnp.where(lane == b, lo, lows[g]))
            new_highs.append(jnp.where(lane == b, hi, highs[g]))
        return tuple(new_lows), tuple(new_highs)

    start = tuple(jnp.zeros((8, 128), f32) for _ in range(VR))
    lows, highs = lax.fori_loop(0, blocks, prepare, (start, start))
    low = jnp.floor(jnp.concatenate(lows, axis=0)).astype(jnp.int32)
    high = jnp.floor(jnp.concatenate(highs, axis=0)).astype(jnp.int32)
    low_v[...] = low
    chunks = (high + 1 - low) // 8 + 1
    num_v[...] = jnp.broadcast_to(jnp.max(chunks, axis=0, keepdims=True), (8, 128))
    c1 = pltpu.make_async_copy(low_v, low_m, sems.at[0])
    c2 = pltpu.make_async_copy(num_v, num_m, sems.at[1])
    c1.start()
    c2.start()
    for c in fetch:
        c.wait()

    first = first_ref[0] * BH - tile * H + H
    last = first + count_ref[0] * BH
    rows = lax.broadcasted_iota(jnp.int32, (3 * H, 128), 0)
    live = (rows >= first) & (rows < last)
    lanes = lax.broadcasted_iota(jnp.int32, (3 * H, 128), 1)
    pages = ((img, 64), (img1, 63))
    zero = jnp.zeros((3 * H, 128), f32)
    lead = GUARD - H
    prev = [zero, zero]
    for k in range(blocks + 1):
        if k < blocks:
            x = jnp.where(live, src_ref[:, 128 * k : 128 * k + 128].astype(f32), 0.0)
        for page, (to, turn) in enumerate(pages):
            now = pltpu.roll(x, turn, 1) if k < blocks else zero
            to[k, 0:lead, :] = jnp.zeros((lead, 128), f32)
            to[k, lead : lead + 3 * H, :] = jnp.where(lanes < turn, prev[page], now)
            to[k, lead + 3 * H :, :] = jnp.zeros((ROWS_HELD - lead - 3 * H, 128), f32)
            prev[page] = now

    c1.wait()
    c2.wait()

    def paint(b, _):
        def chunk(k):
            res = []
            for r in range(H):
                base = low_m[r, b] + 8 * k
                at = pl.ds(jnp.minimum(base + GUARD, ROWS_HELD - 8), 8)
                i0 = jnp.broadcast_to(ix_s[b, r : r + 1, :], (8, 128))
                near = i0 < 128
                m = i0 & 127
                taps = [
                    jnp.where(near, jnp.take_along_axis(page[b, at, :], m, axis=1),
                              jnp.take_along_axis(page[b + 1, at, :], m, axis=1))
                    for page in (img, img1)
                ]
                mixed = taps[0] * w0_s[b, r : r + 1, :] + taps[1] * w1_s[b, r : r + 1, :]
                ty = jnp.maximum(0.0, 1.0 - jnp.abs((sy_s[b, r : r + 1, :] - base.astype(f32)) - subf))
                res.append(jnp.sum(mixed * ty, axis=0, keepdims=True))
            return jnp.concatenate(res, axis=0)

        rowbuf[...] = chunk(0)

        def more(k, _):
            rowbuf[...] += chunk(k)
            return 0

        lax.fori_loop(1, num_m[0, b], more, 0)
        out_ref[:, pl.ds(pl.multiple_of(b * 128, 128), 128)] = rowbuf[...].astype(jnp.bfloat16)
        return 0

    lax.fori_loop(0, blocks, paint, 0)


def render(first, count, fitted, source, wide):
    blocks = W // 128
    vm = pl.BlockSpec(memory_space=pltpu.VMEM)
    sm = pl.BlockSpec(memory_space=pltpu.SMEM)
    hbm = pl.BlockSpec(memory_space=pl.ANY)
    per = lambda d: pltpu.VMEM((blocks, H, 128), d)
    return pl.pallas_call(
        render_kernel,
        out_shape=(
            jax.ShapeDtypeStruct((H, W), jnp.bfloat16),
            jax.ShapeDtypeStruct((6, VR, VC), jnp.float32),
        ),
        in_specs=[sm, sm, vm, hbm, hbm],
        out_specs=(vm, vm),
        scratch_shapes=[
            pltpu.VMEM((3 * H, W), jnp.bfloat16),
            pltpu.VMEM((blocks + 1, ROWS_HELD, 128), jnp.float32),
            pltpu.VMEM((blocks + 1, ROWS_HELD, 128), jnp.float32),
            pltpu.VMEM((blocks, 16, 128), jnp.float32),
            pltpu.VMEM((H, 128), jnp.float32),
            per(jnp.float32), per(jnp.int32), per(jnp.float32), per(jnp.float32),
            pltpu.VMEM((H, 128), jnp.int32),
            pltpu.VMEM((8, 128), jnp.int32),
            pltpu.SMEM((H, 128), jnp.int32),
            pltpu.SMEM((8, 128), jnp.int32),
            pltpu.SemaphoreType.DMA((5,)),
        ],
        name="render",
    )(first, count, fitted, source, wide)


def per_device(points, source, slab_first, slab_count):
    fitted, wide = fit(points, source)
    rendered, affines = render(slab_first, slab_count, fitted, source, wide)
    return (rendered, affines)


def solution(mesh):
    return jax.shard_map(
        per_device,
        mesh=mesh,
        in_specs=(
            P(None, ("sec", "ty")),
            P(("sec", "ty"), None),
            P(("sec", "ty")),
            P(("sec", "ty")),
        ),
        out_specs=(P(("sec", "ty"), None), P(None, ("sec", "ty"), None)),
        check_vma=False,
    )
```

```python
import jax
import jax.numpy as jnp
from jax import lax
from jax.experimental import pallas as pl
from jax.experimental.pallas import tpu as pltpu
from jax.sharding import PartitionSpec as P

W = 2048
BH = 16
SP = 8
H = 32
K = 6
VR = 4
VC = 256


MESH = pl.DeviceIdType.MESH
RIDGE_TERM = 0.01


def solve_affine(moments, vertex_x, vertex_y):
    mass = moments[0]
    mean_px = moments[1] / mass
    mean_py = moments[2] / mass
    mean_qx = moments[3] / mass
    mean_qy = moments[4] / mass
    cov_xx = moments[5] / mass - mean_px * mean_px + RIDGE_TERM
    cov_xy = moments[6] / mass - mean_px * mean_py
    cov_yy = moments[7] / mass - mean_py * mean_py + RIDGE_TERM
    cross_xx = moments[8] / mass - mean_qx * mean_px
    cross_xy = moments[9] / mass - mean_qx * mean_py
    cross_yx = moments[10] / mass - mean_qy * mean_px
    cross_yy = moments[11] / mass - mean_qy * mean_py
    determ = cov_xx * cov_yy - cov_xy * cov_xy
    lin_xx = (cross_xx * cov_yy - cross_xy * cov_xy) / determ
    lin_xy = (cross_xy * cov_xx - cross_xx * cov_xy) / determ
    lin_yx = (cross_yx * cov_yy - cross_yy * cov_xy) / determ
    lin_yy = (cross_yy * cov_xx - cross_yx * cov_xy) / determ
    delta_x = vertex_x - mean_px
    delta_y = vertex_y - mean_py
    shift_x = mean_qx + lin_xx * delta_x + lin_xy * delta_y - vertex_x
    shift_y = mean_qy + lin_yx * delta_x + lin_yy * delta_y - vertex_y
    return [lin_xx, lin_xy, lin_yx, lin_yy, shift_x, shift_y]


OFFSETS = (1, -1, 2, -2)


def fit_kernel(pts_ref, src_ref, fit_ref, wide,
               held, staged, mom, send_p, recv_p, send_s, recv_s, load):
    f32 = jnp.float32
    me = lax.axis_index("ty")
    n = lax.axis_size("ty")
    size = pts_ref.shape[1]
    half = size // 2
    pairs = W // 256

    def exists(d):
        return (me + d >= 0) & (me + d < n)

    own_points = pltpu.make_async_copy(pts_ref, held.at[2], load)
    own_points.start()
    barrier = pltpu.get_barrier_semaphore()
    for d in OFFSETS:
        @pl.when(exists(d))
        def _(d=d):
            pl.semaphore_signal(barrier, inc=1, device_id={"ty": me + d}, device_id_type=MESH)
    peers = sum(exists(d).astype(jnp.int32) for d in OFFSETS)
    pl.semaphore_wait(barrier, peers)
    own_points.wait()

    def points_to(i, d):
        return pltpu.make_async_remote_copy(
            src_ref=held.at[2], dst_ref=held.at[2 - d], send_sem=send_p.at[i], recv_sem=recv_p.at[i],
            device_id={"ty": me + d}, device_id_type=MESH)

    def source_to(i, d):
        return pltpu.make_async_remote_copy(
            src_ref=src_ref, dst_ref=wide.at[i], send_sem=send_s.at[i], recv_sem=recv_s.at[i],
            device_id={"ty": me + d}, device_id_type=MESH)

    for i, d in enumerate(OFFSETS):
        @pl.when(exists(d))
        def _(i=i, d=d):
            points_to(i, d).start()
    for i, d in enumerate(OFFSETS[:2]):
        @pl.when(exists(d))
        def _(i=i, d=d):
            source_to(i, d).start()
    for i, d in enumerate(OFFSETS):
        @pl.when(exists(-d))
        def _(i=i, d=d):
            points_to(i, d).wait_recv()

    spare = jnp.zeros((4, 128), f32)
    for tile in range(5):
        data = held[2] if tile == 2 else jnp.where(exists(tile - 2), held[tile], 0.0)
        for c in range(2):
            row = jnp.concatenate([data[:, c * half : (c + 1) * half], spare], axis=1)
            staged[0, 2 * tile + c] = pltpu.roll(row, 32, 1)
            staged[1, 2 * tile + c] = pltpu.roll(row, half + 96, 1)

    e = lax.broadcasted_iota(jnp.int32, (8, 128), 0)
    own = jnp.where(e == 0, 1, jnp.where(e == 5, 3, 2))
    vy = (((e - 1) * SP + SP // 2) - H // 2).astype(f32) * (1.0 / H)
    lane32 = lax.broadcasted_iota(jnp.int32, (32, 128), 1)
    vert32 = lax.broadcasted_iota(jnp.int32, (32, 128), 0)
    vx32 = (vert32 * SP + SP // 2 - 128).astype(f32) * (1.0 / H)
    centre = (me * H).astype(f32) + H / 2.0

    def group(k, _):
        for odd in range(2):
            pair = 2 * k + odd
            anchor = (pair * 256 + 128).astype(f32)
            block = 2 * pair - 1 + lane32 // 32
            mine = 2 * pair + vert32 // 16
            near = (jnp.abs(block - mine) <= 1) & (block >= 0) & (block < 2 * pairs)
            parts, weights = [], []
            for t in range(10):
                tile = t // 2
                box = staged[odd, t, :, pl.ds(pl.multiple_of(k * 128, 128), 128)]
                px = (box[0:1] - anchor) * (1.0 / H)
                py = (box[1:2] - centre) * (1.0 / H)
                qx = (box[2:3] - anchor) * (1.0 / H)
                qy = (box[3:4] - centre) * (1.0 / H)
                gap = px - vx32
                across = jnp.where(near, jnp.exp(-2.0 * gap * gap), 0.0)
                near_part = across.astype(jnp.bfloat16)
                rest_part = (across - near_part.astype(f32)).astype(jnp.bfloat16)
                weights.append(jnp.concatenate([near_part, rest_part], axis=0))
                rise = py - vy
                there = (jnp.abs(own - tile) <= 1) & exists(tile - 2)
                w = jnp.where(there, jnp.exp(-2.0 * rise * rise), 0.0)
                wpx = w * px
                wpy = w * py
                feats = jnp.concatenate(
                    [w, wpx, wpy, w * qx, w * qy, wpx * px, wpx * py, wpy * py,
                     wpx * qx, wpy * qx, wpx * qy, wpy * qy], axis=0)
                high = feats.astype(jnp.bfloat16)
                low = (feats - high.astype(f32)).astype(jnp.bfloat16)
                parts.append(jnp.concatenate([high, low], axis=0))
            got = lax.dot_general(
                jnp.concatenate(parts, axis=1), jnp.concatenate(weights, axis=1),
                (((1,), (1,)), ((), ())), preferred_element_type=f32)
            got = got[0:96] + got[96:192]
            mom[pair] = got[:, 0:32] + got[:, 32:64]
        return 0

    lax.fori_loop(0, pairs // 2, group, 0)
    moments = [
        jnp.concatenate([mom[g, 8 * f : 8 * f + 8, :] for g in range(pairs)], axis=1) for f in range(12)
    ]
    ew = lax.broadcasted_iota(jnp.int32, (8, VC), 0)
    jw = lax.broadcasted_iota(jnp.int32, (8, VC), 1)
    vertex_y = (((ew - 1) * SP + SP // 2) - H // 2).astype(f32) * (1.0 / H)
    vertex_x = ((jw % 32) * SP + SP // 2 - 128).astype(f32) * (1.0 / H)
    safe = ew < 6
    moments[0] = jnp.where(safe, moments[0], 1.0)
    solved = solve_affine(moments, vertex_x, vertex_y)
    for f in range(6):
        x = solved[f]
        if f >= 4:
            x = jnp.where((ew == 0) & (me == 0), x[1:2], x)
            x = jnp.where((ew == 5) & (me == n - 1), x[4:5], x)
            x = jnp.where(safe, x, 0.0)
        fit_ref[8 * f : 8 * f + 8, :] = x

    for i, d in enumerate(OFFSETS[:2]):
        @pl.when(exists(-d))
        def _(i=i, d=d):
            source_to(i, d).wait_recv()
    for i, d in enumerate(OFFSETS):
        @pl.when(exists(d))
        def _(i=i, d=d):
            points_to(i, d).wait_send()
    for i, d in enumerate(OFFSETS[:2]):
        @pl.when(exists(d))
        def _(i=i, d=d):
            source_to(i, d).wait_send()


def fit(points, source):
    size = points.shape[1]
    vm = pl.BlockSpec(memory_space=pltpu.VMEM)
    return pl.pallas_call(
        fit_kernel,
        out_shape=(
            jax.ShapeDtypeStruct((48, VC), jnp.float32),
            jax.ShapeDtypeStruct((2, H, W), jnp.bfloat16),
        ),
        in_specs=[pl.BlockSpec(memory_space=pl.ANY)] * 2,
        out_specs=(vm, pl.BlockSpec(memory_space=pl.ANY)),
        scratch_shapes=[
            pltpu.VMEM((5, 4, size), jnp.float32),
            pltpu.VMEM((2, 10, 4, size // 2 + 128), jnp.float32),
            pltpu.VMEM((W // 256, 96, 32), jnp.float32),
            pltpu.SemaphoreType.DMA((4,)),
            pltpu.SemaphoreType.DMA((4,)),
            pltpu.SemaphoreType.DMA((2,)),
            pltpu.SemaphoreType.DMA((2,)),
            pltpu.SemaphoreType.DMA,
        ],
        compiler_params=pltpu.CompilerParams(collective_id=0, has_side_effects=True),
        name="fit",
    )(points, source)


GUARD = 40
ROWS_HELD = 144


def split3(x):
    a = x.astype(jnp.bfloat16)
    r = x - a.astype(jnp.float32)
    b = r.astype(jnp.bfloat16)
    c = (r - b.astype(jnp.float32)).astype(jnp.bfloat16)
    return a, b, c


def pick(x, lanes):
    return jnp.take_along_axis(x, lanes, axis=1, mode="promise_in_bounds")


def render_kernel(first_ref, count_ref, fit_ref, own_ref, wide_ref, out_ref, aff_ref,
                  src_ref, img, img1, fine, rowbuf, sy_s, ix_s, w0_s, w1_s, low_v, num_v, low_m, num_m, sems):
    blocks = W // 128
    tile = lax.axis_index("ty")
    f32 = jnp.float32
    fetch = [
        pltpu.make_async_copy(own_ref, src_ref.at[pl.ds(H, H)], sems.at[2]),
        pltpu.make_async_copy(wide_ref.at[0], src_ref.at[pl.ds(0, H)], sems.at[3]),
        pltpu.make_async_copy(wide_ref.at[1], src_ref.at[pl.ds(2 * H, H)], sems.at[4]),
    ]
    for c in fetch:
        c.start()
    for f in range(6):
        aff_ref[f] = fit_ref[8 * f + 1 : 8 * f + 5, :]
    u = fit_ref[32:48, :]
    stacked = jnp.concatenate([p.astype(f32) for p in split3(u)], axis=0).astype(jnp.bfloat16)
    for part in range(W // 256):
        col = lax.broadcasted_iota(jnp.int32, (VC, 256), 1) + part * 256
        col = jnp.clip(col, SP // 2, W - SP // 2)
        ver = lax.broadcasted_iota(jnp.int32, (VC, 256), 0) * SP + SP // 2
        tent = jnp.maximum(0.0, 1.0 - jnp.abs(col - ver).astype(f32) * (1.0 / SP)).astype(jnp.bfloat16)
        got = jnp.dot(stacked, tent, preferred_element_type=f32)
        got = got[0:16] + got[16:32] + got[32:48]
        fine[2 * part] = got[:, :128]
        fine[2 * part + 1] = got[:, 128:]

    sub = lax.broadcasted_iota(jnp.int32, (8, 128), 0)
    subf = sub.astype(f32)
    lane = lax.broadcasted_iota(jnp.int32, (8, 128), 1)
    wa = jnp.maximum(0.0, 1.0 - (subf + 4.0) * (1.0 / SP))
    wb = jnp.maximum(0.0, 1.0 - jnp.abs(subf - 4.0) * (1.0 / SP))
    wc = jnp.maximum(0.0, 1.0 - (12.0 - subf) * (1.0 / SP))
    lanef = lane.astype(f32)

    def prepare(b, carry):
        lows, highs = carry
        f = fine[b]
        new_lows, new_highs = [], []
        for g in range(VR):
            dx = wa * f[g : g + 1] + wb * f[g + 1 : g + 2] + wc * f[g + 2 : g + 3]
            dy = wa * f[g + 8 : g + 9] + wb * f[g + 9 : g + 10] + wc * f[g + 10 : g + 11]
            sy = jnp.clip(subf + (8.0 * g) + H * dy, -33.0, 64.0)
            sx = (lanef + (b * 128).astype(f32)) + H * dx
            lx = jnp.clip(sx - (b * 128 - 64).astype(f32), -1.0, 256.0)
            base = jnp.floor(lx)
            frac = lx - base
            ix = base.astype(jnp.int32)
            w0 = jnp.where(ix < 0, frac, jnp.where(ix < 256, 1.0 - frac, 0.0)).astype(jnp.bfloat16).astype(f32)
            w1 = jnp.where((ix >= 0) & (ix < 255), frac, 0.0).astype(jnp.bfloat16).astype(f32)
            r = slice(8 * g, 8 * g + 8)
            sy_s[b, r, :] = sy
            ix_s[b, r, :] = jnp.clip(ix, 0, 255)
            w0_s[b, r, :] = w0
            w1_s[b, r, :] = w1
            lo = jnp.min(sy, axis=1, keepdims=True)
            hi = jnp.max(sy, axis=1, keepdims=True)
            new_lows.append(jnp.where(lane == b, lo, lows[g]))
            new_highs.append(jnp.where(lane == b, hi, highs[g]))
        return tuple(new_lows), tuple(new_highs)

    start = tuple(jnp.zeros((8, 128), f32) for _ in range(VR))
    lows, highs = lax.fori_loop(0, blocks, prepare, (start, start))
    low = jnp.floor(jnp.concatenate(lows, axis=0)).astype(jnp.int32)
    high = jnp.floor(jnp.concatenate(highs, axis=0)).astype(jnp.int32)
    low_v[...] = low
    chunks = (high + 1 - low) // 8 + 1
    num_v[...] = jnp.broadcast_to(jnp.max(chunks, axis=0, keepdims=True), (8, 128))
    c1 = pltpu.make_async_copy(low_v, low_m, sems.at[0])
    c2 = pltpu.make_async_copy(num_v, num_m, sems.at[1])
    c1.start()
    c2.start()
    for c in fetch:
        c.wait()

    first = first_ref[0] * BH - tile * H + H
    last = first + count_ref[0] * BH
    rows = lax.broadcasted_iota(jnp.int32, (3 * H, 128), 0)
    live = (rows >= first) & (rows < last)
    lanes = lax.broadcasted_iota(jnp.int32, (3 * H, 128), 1)
    pages = ((img, 64), (img1, 63))
    zero = jnp.zeros((3 * H, 128), f32)
    lead = GUARD - H
    prev = [zero, zero]
    for k in range(blocks + 1):
        if k < blocks:
            x = jnp.where(live, src_ref[:, 128 * k : 128 * k + 128].astype(f32), 0.0)
        for page, (to, turn) in enumerate(pages):
            now = pltpu.roll(x, turn, 1) if k < blocks else zero
            to[k, 0:lead, :] = jnp.zeros((lead, 128), f32)
            to[k, lead : lead + 3 * H, :] = jnp.where(lanes < turn, prev[page], now)
            to[k, lead + 3 * H :, :] = jnp.zeros((ROWS_HELD - lead - 3 * H, 128), f32)
            prev[page] = now

    c1.wait()
    c2.wait()

    def paint(b, _):
        def chunk(k):
            res = []
            for r in range(H):
                base = low_m[r, b]
                at = base + GUARD
                if not (isinstance(k, int) and k == 0):
                    base = base + 8 * k
                    at = jnp.minimum(base + GUARD, ROWS_HELD - 8)
                at = pl.ds(at, 8)
                i0 = jnp.broadcast_to(ix_s[b, r : r + 1, :], (8, 128))
                near = i0 < 128
                m = i0 & 127
                taps = [
                    jnp.where(near, pick(page[b, at, :], m), pick(page[b + 1, at, :], m))
                    for page in (img, img1)
                ]
                mixed = taps[0] * w0_s[b, r : r + 1, :] + taps[1] * w1_s[b, r : r + 1, :]
                ty = jnp.maximum(0.0, 1.0 - jnp.abs((sy_s[b, r : r + 1, :] - base.astype(f32)) - subf))
                res.append(jnp.sum(mixed * ty, axis=0, keepdims=True))
            return jnp.concatenate(res, axis=0)

        rowbuf[...] = chunk(0)

        def more(k, _):
            rowbuf[...] += chunk(k)
            return 0

        lax.fori_loop(1, num_m[0, b], more, 0)
        out_ref[:, pl.ds(pl.multiple_of(b * 128, 128), 128)] = rowbuf[...].astype(jnp.bfloat16)
        return 0

    lax.fori_loop(0, blocks, paint, 0)


def render(first, count, fitted, source, wide):
    blocks = W // 128
    vm = pl.BlockSpec(memory_space=pltpu.VMEM)
    sm = pl.BlockSpec(memory_space=pltpu.SMEM)
    hbm = pl.BlockSpec(memory_space=pl.ANY)
    per = lambda d: pltpu.VMEM((blocks, H, 128), d)
    return pl.pallas_call(
        render_kernel,
        out_shape=(
            jax.ShapeDtypeStruct((H, W), jnp.bfloat16),
            jax.ShapeDtypeStruct((6, VR, VC), jnp.float32),
        ),
        in_specs=[sm, sm, vm, hbm, hbm],
        out_specs=(vm, vm),
        scratch_shapes=[
            pltpu.VMEM((3 * H, W), jnp.bfloat16),
            pltpu.VMEM((blocks + 1, ROWS_HELD, 128), jnp.float32),
            pltpu.VMEM((blocks + 1, ROWS_HELD, 128), jnp.float32),
            pltpu.VMEM((blocks, 16, 128), jnp.float32),
            pltpu.VMEM((H, 128), jnp.float32),
            per(jnp.float32), per(jnp.int32), per(jnp.float32), per(jnp.float32),
            pltpu.VMEM((H, 128), jnp.int32),
            pltpu.VMEM((8, 128), jnp.int32),
            pltpu.SMEM((H, 128), jnp.int32),
            pltpu.SMEM((8, 128), jnp.int32),
            pltpu.SemaphoreType.DMA((5,)),
        ],
        name="render",
    )(first, count, fitted, source, wide)


def per_device(points, source, slab_first, slab_count):
    fitted, wide = fit(points, source)
    rendered, affines = render(slab_first, slab_count, fitted, source, wide)
    return (rendered, affines)


def solution(mesh):
    return jax.shard_map(
        per_device,
        mesh=mesh,
        in_specs=(
            P(None, ("sec", "ty")),
            P(("sec", "ty"), None),
            P(("sec", "ty")),
            P(("sec", "ty")),
        ),
        out_specs=(P(("sec", "ty"), None), P(None, ("sec", "ty"), None)),
        check_vma=False,
    )
```
